32 devices in a mesh: tm: 2 (over x), gx: 4 (over z), gy: 4 (over y, core).
Axes of the slice: x: 2, y: 2, z: 4, core: 2. Of those that a mesh axis runs over, the one named last changes fastest.
Arguments:
- increment: float32 [2, 137, 64, 512], P('tm', None, 'gx', 'gy'), may hold values from -6 to 6
- dual_state: float32 [2, 137, 64, 512], P('tm', None, 'gx', 'gy'), may hold values from -6 to 6
- forcing: float32 [2, 137, 64, 512], P('tm', None, 'gx', 'gy'), may hold values from -6 to 6
- gradient: float32 [2, 137, 64, 512], P('tm', None, 'gx', 'gy'), may hold values from -3 to 3
- courant_x: float32 [2, 137, 64, 512], P('tm', None, 'gx', 'gy'), may hold values from 0.05 to 0.3
- courant_y: float32 [2, 137, 64, 512], P('tm', None, 'gx', 'gy'), may hold values from 0.05 to 0.3
- error_var: float32 [2, 137, 64, 512], P('tm', None, 'gx', 'gy'), may hold values from 0.2 to 2
- obs_weight: float32 [2, 137, 64, 512], P('tm', None, 'gx', 'gy'), may hold values from 0.2 to 2
- diffusion: float32 [137], replicated, may hold values from 0.02 to 0.1
- level_mix: float32 [137, 137], replicated, may hold values from -0.5 to 0.8
Outputs:
- dual_next: float32 [2, 137, 64, 512], P('tm', None, 'gx', 'gy')
- increment_next: float32 [2, 137, 64, 512], P('tm', None, 'gx', 'gy')
The draws below stay inside these ranges and needn't reach their ends.
All inputs are finite; a program needn't handle non-finite values.
Results may differ from the reference program's by a relative error of at most 0.0001.
Values sent between devices are 32-bit elements; how exact they have to be, the bound alone decides.
No kernel may reach another device: no remote copies, remote signals or barrier semaphores. Data moves between devices by JAX's collectives and lax.ppermute only.
A program may use at most 128 MiB of HBM per device.

```python
import math
import jax
import jax.numpy as jnp
from jax import lax

LEVELS = 137
STEPS = 3
SUBWIN = 2
NX = 64
NY = 512


def coherent_field(key):
    level_place = ((jnp.arange(LEVELS, dtype=jnp.float32) + 0.5) / LEVELS)[None, :, None, None]
    along_x = (jnp.arange(NX, dtype=jnp.float32) / NX)[None, None, :, None]
    along_y = (jnp.arange(NY, dtype=jnp.float32) / NY)[None, None, None, :]
    window_place = jnp.arange(SUBWIN, dtype=jnp.float32) / max(SUBWIN - 1, 1)
    window_scale = (0.6 + 0.4 * window_place)[:, None, None, None]
    summed = jnp.zeros((SUBWIN, LEVELS, NX, NY), jnp.float32)
    for mode in range(3):
        mode_key = jax.random.fold_in(key, 31 + mode)
        mode_keys = jax.random.split(mode_key, 6)
        wave_x = jax.random.randint(mode_keys[0], (), 1, 3).astype(jnp.float32)
        wave_y = jax.random.randint(mode_keys[1], (), 1, 3).astype(jnp.float32)
        wave_level = jax.random.randint(mode_keys[2], (), 0, 3).astype(jnp.float32)
        phases = jax.random.uniform(mode_keys[3], (3,), jnp.float32, -math.pi, math.pi)
        strength = jax.random.uniform(mode_keys[4], (), jnp.float32, 0.6, 1.0)
        jitter = 1.0 + 0.1 * jax.random.uniform(mode_keys[5], (SUBWIN, 1, 1, 1), jnp.float32, -1.0, 1.0)
        pattern = jnp.cos(2.0 * math.pi * wave_x * along_x + phases[0])
        pattern = pattern * jnp.cos(2.0 * math.pi * wave_y * along_y + phases[1])
        pattern = pattern * jnp.cos(math.pi * wave_level * level_place + phases[2])
        summed = summed + strength * jitter * pattern
    rough_key = jax.random.fold_in(key, 97)
    smooth = 1.4 * summed
    roughness = 0.5 * jnp.clip(jax.random.normal(rough_key, (SUBWIN, LEVELS, NX, NY), jnp.float32), -2.5, 2.5)
    return window_scale * smooth + roughness


def draw_increment(key, part):
    return coherent_field(jax.random.fold_in(key, 101))


def draw_dual_state(key, part):
    return coherent_field(jax.random.fold_in(key, 202))


def draw_forcing(key, part):
    normal_part = 0.5 * jnp.clip(jax.random.normal(key, (SUBWIN, LEVELS, NX, NY), jnp.float32), -4.0, 4.0)
    growth = 1.0 + 2.0 * jnp.arange(SUBWIN, dtype=jnp.float32) / max(SUBWIN - 1, 1)
    growth = growth[:, None, None, None]
    return normal_part * growth


def draw_level_mix(key, part):
    key_diag = jax.random.fold_in(key, 11)
    key_coupling = jax.random.fold_in(key, 23)
    diagonal = jax.random.uniform(key_diag, (LEVELS,), jnp.float32, 0.5, 0.8)
    coupling = jnp.clip(jax.random.normal(key_coupling, (LEVELS, LEVELS), jnp.float32), -6.0, 6.0) * (0.3 / math.sqrt(LEVELS))
    coupling = coupling * (1.0 - jnp.eye(LEVELS, dtype=jnp.float32))
    return coupling + jnp.diag(diagonal)


def block_levels(key, shape, cuts, least, high):
    loudness, own = 1.0, jax.random.fold_in(key, 6)
    for position, blocks in cuts:
        draws = jnp.exp(jax.random.uniform(jax.random.fold_in(own, position), (blocks,), jnp.float32, least / len(cuts), high / len(cuts)))
        loudness = loudness * jnp.repeat(draws, shape[position] // blocks).reshape([-1 if axis == position else 1 for axis in range(len(shape))])
    return loudness


def bell_draw(stream_key, dims, width, limit, cuts=(), kind=jnp.bfloat16):
    entries = jax.random.normal(stream_key, dims, jnp.float32) * width
    if len(cuts) > 0:
        entries = block_levels(stream_key, dims, cuts, -0.22, 0.18) * entries
    return jnp.clip(entries, min=-limit, max=limit).astype(kind)


def setup_inputs(seed: int = 0) -> dict:
    arg_keys = jax.random.split(jax.random.key(seed), 11)
    increment = draw_increment(jax.random.fold_in(arg_keys[10], 71), 0)
    dual_state = draw_dual_state(jax.random.fold_in(arg_keys[10], 71), 0)
    forcing = draw_forcing(jax.random.fold_in(arg_keys[10], 71), 0)
    gradient = bell_draw(arg_keys[3], (SUBWIN, LEVELS, NX, NY), 0.5, 3.0, ((0, 2), (2, 4), (3, 4)), jnp.float32)
    courant_x = jnp.clip(0.05 + 0.25 * jax.random.uniform(arg_keys[4], (SUBWIN, LEVELS, NX, NY), jnp.float32) ** block_levels(arg_keys[4], (SUBWIN, LEVELS, NX, NY), ((0, 2), (2, 4), (3, 4)), -0.2, 0.2), 0.05, 0.3)
    courant_y = jnp.clip(0.05 + 0.25 * jax.random.uniform(arg_keys[5], (SUBWIN, LEVELS, NX, NY), jnp.float32) ** block_levels(arg_keys[5], (SUBWIN, LEVELS, NX, NY), ((0, 2), (2, 4), (3, 4)), -0.2, 0.2), 0.05, 0.3)
    error_var = jnp.clip(jnp.exp(math.log(2.0) - 2.3025851 * jax.random.uniform(arg_keys[6], (SUBWIN, LEVELS, NX, NY), jnp.float32) ** block_levels(arg_keys[6], (SUBWIN, LEVELS, NX, NY), ((0, 2), (2, 4), (3, 4)), -0.2, 0.2)), 0.2, 2.0)
    obs_weight = jnp.clip(jnp.exp(math.log(2.0) - 2.3025851 * jax.random.uniform(arg_keys[7], (SUBWIN, LEVELS, NX, NY), jnp.float32) ** block_levels(arg_keys[7], (SUBWIN, LEVELS, NX, NY), ((0, 2), (2, 4), (3, 4)), -0.2, 0.2)), 0.2, 2.0)
    diffusion = jnp.clip(jnp.exp(jax.random.uniform(arg_keys[8], (LEVELS,), jnp.float32, math.log(0.02), math.log(0.1))), 0.02, 0.1)
    level_mix = draw_level_mix(jax.random.fold_in(arg_keys[10], 71), 0)
    return dict(increment=increment, dual_state=dual_state, forcing=forcing, gradient=gradient, courant_x=courant_x, courant_y=courant_y, error_var=error_var, obs_weight=obs_weight, diffusion=diffusion, level_mix=level_mix)


def apply_levels(matrix, current):
    return jnp.einsum('lm,mxy->lxy', matrix, current, precision=lax.Precision.HIGHEST)

def neighbours(current):
    padded = jnp.pad(current, ((0, 0), (1, 1), (1, 1)))
    return (padded[:, :-2, 1:-1], padded[:, 2:, 1:-1], padded[:, 1:-1, :-2], padded[:, 1:-1, 2:])

def tangent_step(current, courant_x, courant_y, lower_x, lower_y, spread, level_mix):
    minus_x, plus_x, minus_y, plus_y = neighbours(current)
    advected = (1.0 - courant_x - courant_y - 4.0 * spread) * current + lower_x * minus_x + lower_y * minus_y
    advected = advected + spread * (minus_x + plus_x + minus_y + plus_y)
    return apply_levels(level_mix, advected)

def adjoint_step(current, courant_x, courant_y, spread, level_mix):
    mixed_back = apply_levels(level_mix.T, current)
    minus_x, plus_x, minus_y, plus_y = neighbours(mixed_back)
    result = (1.0 - courant_x - courant_y - 4.0 * spread) * mixed_back + courant_x * plus_x + courant_y * plus_y
    return result + spread * (minus_x + plus_x + minus_y + plus_y)

def reference(increment, dual_state, forcing, gradient, courant_x, courant_y, error_var, obs_weight, diffusion, level_mix):
    spread = diffusion[:, None, None]
    windows = increment.shape[0]
    end_states = []
    back_states = []
    for window in range(windows):
        flow_x = courant_x[window]
        flow_y = courant_y[window]
        lower_x = jnp.pad(flow_x, ((0, 0), (1, 0), (0, 0)))[:, :-1, :]
        lower_y = jnp.pad(flow_y, ((0, 0), (0, 0), (1, 0)))[:, :, :-1]
        forward_state = increment[window]
        for substep in range(STEPS):
            forward_state = tangent_step(forward_state, flow_x, flow_y, lower_x, lower_y, spread, level_mix)
        end_states.append(forward_state)
        if window + 1 < windows:
            adjoint_state = dual_state[window + 1]
        else:
            adjoint_state = jnp.zeros_like(dual_state[0])
        for substep in range(STEPS):
            adjoint_state = adjoint_step(adjoint_state, flow_x, flow_y, spread, level_mix)
        back_states.append(adjoint_state)
    earlier_end = jnp.stack([jnp.zeros_like(increment[0])] + end_states[:-1])
    back_all = jnp.stack(back_states)
    residual_dual = forcing - error_var * dual_state - increment + earlier_end
    residual_incr = gradient - obs_weight * increment - dual_state + back_all
    global_sum = jnp.sum(residual_dual * residual_dual) + jnp.sum(residual_incr * residual_incr)
    cell_count = 2 * residual_dual.size
    root_mean = jnp.sqrt(global_sum / cell_count + 1e-06)
    step_scale = jnp.minimum(1.0, 0.5 / root_mean)
    return (dual_state + step_scale * residual_dual, increment + step_scale * residual_incr)
```

```python
import functools

import jax
import jax.numpy as jnp
from jax import lax
from jax.experimental import pallas as pl
from jax.experimental.pallas import tpu as pltpu
from jax.sharding import PartitionSpec as P

STEPS = 3
LANES = 128
PITCH = 3 * STEPS
F32 = jnp.float32
BF16 = jnp.bfloat16


def sds(*shape, dtype=F32):
    return jax.ShapeDtypeStruct(shape, dtype)


def call(body, outs, args, name):
    return pl.pallas_call(
        body,
        out_shape=outs,
        in_specs=[pl.BlockSpec(memory_space=pltpu.VMEM)] * len(args),
        out_specs=jax.tree.map(lambda _: pl.BlockSpec(memory_space=pltpu.VMEM), outs),
        name=name,
    )(*args)


def split(value):
    high = value.astype(BF16)
    return high, (value - high.astype(F32)).astype(BF16)


def mix(matrix, value):
    levels = value.shape[0]
    stride = matrix.shape[0] // 2
    high, low = split(value)
    both = jnp.dot(matrix[...], high, preferred_element_type=F32)
    last = jnp.dot(matrix[0:levels, :], low, preferred_element_type=F32)
    return both[0:levels] + (both[stride : stride + levels] + last)


def pairs(keys):
    keys = list(keys)
    return [keys[i : i + 2] for i in range(0, len(keys), 2)]


def mix_rows(matrix, rows):
    out = {}
    for group in pairs(sorted(rows)):
        wide = jnp.concatenate([rows[x] for x in group], axis=1) if len(group) > 1 else rows[group[0]]
        mixed = mix(matrix, wide)
        for place, x in enumerate(group):
            out[x] = mixed[:, place * LANES : (place + 1) * LANES]
    return out


def natural(ref, x, depth, levels):
    return ref[pl.ds(x, levels, stride=depth), :]


def forward_row(v, a, b, s, x):
    here = v(x)
    out = (1.0 - a(x) - b(x) - 4.0 * s) * here
    out = out + (a(x - 1) + s) * v(x - 1) + s * v(x + 1)
    out = out + pltpu.roll((b(x) + s) * here, 1, 1)
    return out + s * pltpu.roll(here, LANES - 1, 1)


def adjoint_row(w, a, b, s, x):
    here = w(x)
    ax = a(x)
    bx = b(x)
    out = (1.0 - ax - bx - 4.0 * s) * here
    out = out + (ax + s) * w(x + 1) + s * w(x - 1)
    out = out + (bx + s) * pltpu.roll(here, LANES - 1, 1)
    return out + s * pltpu.roll(here, 1, 1)


def edge(axis, last):
    here = lax.axis_index(axis)
    return here == (lax.axis_size(axis) - 1 if last else 0)


def prepare_body(X, L, v, a, b, d, m, low, high, near, core, mats, matst):
    row = lambda ref, x: natural(ref, x, X, L)
    H = STEPS
    for i in range(H):
        near[i] = row(d, i)
        near[H + i] = row(d, X - H + i)
    for i in range(X - 2 * H):
        core[i] = row(d, H + i)
    for i in range(H):
        low[i] = row(v, i)
        high[i] = row(v, X - H + i)
    for i in range(H - 1):
        low[H + i] = row(a, i)
        low[2 * H - 1 + i] = row(b, i)
        high[2 * H + i] = row(b, X - H + 1 + i)
    for i in range(H):
        high[H + i] = row(a, X - H + i)
    half = mats.shape[0] // 2
    for value, ref in ((m[...], mats), (m[...].T, matst)):
        upper, lower = split(value)
        ref[0:L] = upper
        ref[half : half + L] = lower


def core_body(X, L, v, a, b, sref, mats, tv, ta, tb, end, mid, one, two):
    H = STEPS
    s = jnp.broadcast_to(sref[...], (L, LANES))
    for x in range(X):
        for src, dst in ((v, tv), (a, ta), (b, tb)):
            dst[x] = natural(src, x, X, L)
    levels = [lambda x: tv[x], lambda x: one[x], lambda x: two[x]]
    for step in range(H):
        for group in pairs(range(step + 1, X - step - 1)):
            rows = {x: forward_row(levels[step], lambda x: ta[x], lambda x: tb[x], s, x) for x in group}
            for x, value in mix_rows(mats, rows).items():
                if step == 0:
                    one[x] = value
                elif step == 1:
                    two[x] = value
                else:
                    end[x - H] = value
    for place, (ref, x) in enumerate(
        ((one, 1), (one, 2), (one, X - 3), (one, X - 2), (two, 2), (two, 3), (two, X - 4), (two, X - 3))
    ):
        mid[place] = ref[x]


def halo_fields(X, top, bot, tv, ta, tb):
    H = STEPS

    def v(x):
        return top[x + H] if x < 0 else (bot[x - X] if x >= X else tv[x])

    def a(x):
        return top[2 * H + x] if x < 0 else (bot[H + x - X] if x >= X else ta[x])

    def b(x):
        return top[3 * H - 1 + x] if x < 0 else (bot[2 * H - 1 + x - X] if x >= X else tb[x])

    return v, a, b


def rim_body(X, L, tv, ta, tb, top, bot, mid, sref, mats, out):
    H = STEPS
    s = jnp.broadcast_to(sref[...], (L, LANES))
    v, a, b = halo_fields(X, top, bot, tv, ta, tb)
    first = edge("gx", False)
    final = edge("gx", True)
    known = [
        {},
        {1: 0, 2: 1, X - 3: 2, X - 2: 3},
        {2: 4, 3: 5, X - 4: 6, X - 3: 7},
    ]
    state = None
    for step in range(H):
        got = state

        def current(x):
            if step == 0:
                return v(x)
            return mid[known[step][x]] if x in known[step] else got[x]

        reach = H - 1 - step
        rows = {}
        for x in list(range(-reach, H - reach)) + list(range(X - H + reach, X + reach)):
            rows[x] = forward_row(current, a, b, s, x)
        state = mix_rows(mats, rows)
        for x in state:
            if x < 0:
                state[x] = jnp.where(first, 0.0, state[x])
            if x >= X:
                state[x] = jnp.where(final, 0.0, state[x])
    for i in range(H):
        out[i] = state[i]
        out[H + i] = state[X - H + i]


def seam_gather(X, L, field, present):
    H = STEPS
    lane = lax.broadcasted_iota(jnp.int32, (L, LANES), 1)
    tiles = 2
    left = [jnp.zeros((L, LANES), F32) for _ in range(tiles)]
    right = [jnp.zeros((L, LANES), F32) for _ in range(tiles)]
    for r in range(X + 2 * H):
        x = r - H
        if not present(x):
            continue
        begin = PITCH * r
        rolled = pltpu.roll(field(x), (begin + 2 * H) % LANES, 1)
        for t in range(tiles):
            at = begin - t * LANES
            if at < LANES and at + 2 * H > 0:
                right[t] = jnp.where((lane >= at) & (lane < at + 2 * H), rolled, right[t])
            at += 2 * H
            if at < LANES and at + 2 * H > 0:
                left[t] = jnp.where((lane >= at) & (lane < at + 2 * H), rolled, left[t])
    return jnp.concatenate(left, axis=1), jnp.concatenate(right, axis=1)


def third(L, which):
    lane = lax.broadcasted_iota(jnp.int32, (L, 2 * LANES), 1)
    return lax.rem(lane, PITCH) // STEPS == which


def roll(value, shift):
    return pltpu.roll(value, shift % value.shape[1], 1)


def pack_body(X, L, tv, ta, tb, top, bot, own, to_right, to_left):
    H = STEPS
    v, a, b = halo_fields(X, top, bot, tv, ta, tb)
    lv, rv = seam_gather(X, L, v, lambda x: True)
    la, ra = seam_gather(X, L, a, lambda x: x < X + H - 1)
    lb, rb = seam_gather(X, L, b, lambda x: -H < x < X + H - 1)
    for place, value in enumerate((lv, rv, la, ra, lb, rb)):
        own[place] = value
    to_right[...] = jnp.where(third(L, 1), rv, jnp.where(third(L, 2), roll(ra, H), roll(rb, 2 * H)))
    to_left[...] = jnp.where(third(L, 2), lv, jnp.where(third(L, 0), roll(la, H), roll(lb, 2 * H)))


def seam_masks(X, L):
    H = STEPS
    lane = lax.broadcasted_iota(jnp.int32, (L, 2 * LANES), 1)
    up, down = edge("gx", False), edge("gx", True)
    rows = (up & (lane < PITCH * H)), (down & (lane >= PITCH * (X + H)))
    left_rows = (up & (lane < PITCH * H + H)), (down & (lane >= PITCH * (X + H) + H))
    left = left_rows[0] | left_rows[1] | (edge("gy", False) & third(L, 1))
    right = rows[0] | rows[1] | (edge("gy", True) & third(L, 2))
    return left, right


def forward_seam(v, a, b, s, matrix):
    out = (1.0 - a - b - 4.0 * s) * v + s * (roll(v, -PITCH) + roll(v, -1))
    out = out + roll((a + s) * v, PITCH) + roll((b + s) * v, 1)
    return mix(matrix, out)


def adjoint_seam(u, a, b, s, matrix):
    w = mix(matrix, u)
    out = (1.0 - a - b - 4.0 * s) * w + s * (roll(w, PITCH) + roll(w, 1))
    return out + (a + s) * roll(w, -PITCH) + (b + s) * roll(w, -1)


def seam_body(X, L, own, from_left, from_right, sref, mats, out, coef):
    H = STEPS
    s = jnp.broadcast_to(sref[...], (L, 2 * LANES))
    lo, hi = from_left[...], from_right[...]
    lv = jnp.where(third(L, 1), lo, own[0])
    rv = jnp.where(third(L, 2), hi, own[1])
    coef[0] = jnp.where(third(L, 1), roll(lo, -H), own[2])
    coef[1] = jnp.where(third(L, 2), roll(hi, -H), own[3])
    coef[2] = jnp.where(third(L, 1), roll(lo, -2 * H), own[4])
    coef[3] = jnp.where(third(L, 2), roll(hi, -2 * H), own[5])
    left_out, right_out = seam_masks(X, L)
    for step in range(H):
        lv = jnp.where(left_out, 0.0, forward_seam(lv, coef[0], coef[2], s, mats))
        rv = jnp.where(right_out, 0.0, forward_seam(rv, coef[1], coef[3], s, mats))
    out[...] = jnp.where(third(L, 1), rv, lv)


def dual_rows(X, near, core, top, bot):
    H = STEPS

    def u(x):
        if x < 0:
            return top[x + H]
        if x >= X:
            return bot[x - X]
        if x < H:
            return near[x]
        if x >= X - H:
            return near[H + x - (X - H)]
        return core[x - H]

    return u


def pack_dual_body(X, L, near, core, top, bot, left, right):
    left[...], right[...] = seam_gather(X, L, dual_rows(X, near, core, top, bot), lambda x: True)


def adjoint_body(X, L, near, core, utop, ubot, ta, tb, top, bot, sref, mats, out, wide, state):
    H = STEPS
    s = jnp.broadcast_to(sref[...], (L, LANES))
    _, a, b = halo_fields(X, top, bot, ta, ta, tb)
    u0 = dual_rows(X, near, core, utop, ubot)
    first = edge("gx", False)
    final = edge("gx", True)
    for step in range(H):
        reach = H - step
        source = u0 if step == 0 else (lambda x: state[x + H])
        for group in pairs(range(-reach, X + reach)):
            rows = mix_rows(mats, {x: source(x) for x in group})
            for x, value in rows.items():
                wide[x + H] = value
        for x in range(1 - reach, X + reach - 1):
            value = adjoint_row(lambda x: wide[x + H], a, b, s, x)
            if x < 0:
                value = jnp.where(first, 0.0, value)
            if x >= X:
                value = jnp.where(final, 0.0, value)
            if step == H - 1:
                out[x] = value
            else:
                state[x + H] = value


def adjoint_seam_body(X, L, left, right, from_left, from_right, coef, sref, mats, out):
    H = STEPS
    s = jnp.broadcast_to(sref[...], (L, 2 * LANES))
    lu = jnp.where(third(L, 1), from_left[...], left[...])
    ru = jnp.where(third(L, 2), from_right[...], right[...])
    left_out, right_out = seam_masks(X, L)
    for step in range(H):
        lu = jnp.where(left_out, 0.0, adjoint_seam(lu, coef[0], coef[2], s, mats))
        ru = jnp.where(right_out, 0.0, adjoint_seam(ru, coef[1], coef[3], s, mats))
    out[...] = jnp.where(third(L, 1), ru, lu)


def merged_row(X, L, row, seam, x):
    H = STEPS
    at = PITCH * (x + H) + H
    tile = at // LANES
    lane = lax.broadcasted_iota(jnp.int32, (L, LANES), 1)
    part = seam[:, tile * LANES : (tile + 1) * LANES]
    rolled = pltpu.roll(part, (LANES - H - at) % LANES, 1)
    return jnp.where((lane < H) | (lane >= LANES - H), rolled, row)


def residual_body(
    X, L, ecore, enear, eseam, back, bseam, force, var, dual, incr, grad, obs, rdual, rincr, part, end, adj
):
    H = STEPS
    for x in range(X):
        row = ecore[x - H] if H <= x < X - H else enear[x if x < H else x - X + 2 * H]
        end[pl.ds(x, L, stride=X), :] = merged_row(X, L, row, eseam, x)
        adj[pl.ds(x, L, stride=X), :] = merged_row(X, L, back[x], bseam, x)
    rd = force[...] - var[...] * dual[...] - incr[...] + end[...]
    rdual[...] = rd
    ri = grad[...] - obs[...] * incr[...] - dual[...] + adj[...]
    rincr[...] = ri
    part[...] = jnp.broadcast_to(jnp.sum(rd * rd + ri * ri, keepdims=True), part.shape)


def update_body(count, parts, dual, incr, rdual, rincr, dnext, inext):
    total = jnp.sum(parts[:, 0:1], keepdims=True)
    scale = jnp.minimum(1.0, 0.5 / jnp.sqrt(total * (1.0 / count) + 1e-06))
    dnext[...] = dual[...] + scale * rdual[...]
    inext[...] = incr[...] + scale * rincr[...]


def shifted(block, axis, distance):
    devices = range(lax.axis_size(axis))
    return lax.ppermute(block, axis, [(i - distance, i) for i in devices if i - distance in devices])


def local(increment, dual_state, forcing, gradient, courant_x, courant_y, error_var, obs_weight, diffusion, level_mix):
    _, L, X, Y = increment.shape
    assert Y == LANES and X % 8 == 0 and PITCH * (X + 2 * STEPS) + STEPS <= 2 * LANES
    H = STEPS
    half = -(-L // 16) * 16
    flat = lambda t: t.reshape(L * X, Y)
    v, d, a, b = flat(increment), flat(dual_state), flat(courant_x), flat(courant_y)
    s = diffusion[:, None]
    bind = lambda body: functools.partial(body, X, L)
    plane = lambda n: sds(n, L, LANES)
    seam = sds(L, 2 * LANES)

    low, high, near, core, mats, matst = call(
        bind(prepare_body),
        (plane(3 * H - 2), plane(3 * H - 1), plane(2 * H), plane(X - 2 * H),
         sds(2 * half, L, dtype=BF16), sds(2 * half, L, dtype=BF16)),
        (v, a, b, d, level_mix), "prepare")
    near = shifted(near, "tm", -1)
    core = shifted(core, "tm", -1)
    top = shifted(high, "gx", 1)
    bot = shifted(low, "gx", -1)

    tv, ta, tb, ecore, mid = pl.pallas_call(
        bind(core_body),
        out_shape=(plane(X), plane(X), plane(X), plane(X - 2 * H), plane(8)),
        in_specs=[pl.BlockSpec(memory_space=pltpu.VMEM)] * 5,
        out_specs=(pl.BlockSpec(memory_space=pltpu.VMEM),) * 5,
        scratch_shapes=[pltpu.VMEM((X, L, LANES), F32)] * 2,
        name="core",
    )(v, a, b, s, mats)
    ecore = shifted(ecore, "tm", 1)

    own, to_right, to_left = call(bind(pack_body), (sds(6, L, 2 * LANES), seam, seam), (tv, ta, tb, top, bot), "pack")
    from_left = shifted(to_right, "gy", 1)
    from_right = shifted(to_left, "gy", -1)
    enear = call(bind(rim_body), plane(2 * H), (tv, ta, tb, top, bot, mid, s, mats), "rim")
    enear = shifted(enear, "tm", 1)
    eseam, coef = call(bind(seam_body), (seam, sds(4, L, 2 * LANES)), (own, from_left, from_right, s, mats), "seam")
    eseam = shifted(eseam, "tm", 1)

    utop = shifted(near[H:], "gx", 1)
    ubot = shifted(near[:H], "gx", -1)
    uleft, uright = call(bind(pack_dual_body), (seam, seam), (near, core, utop, ubot), "pack_dual")
    ufrom_left = shifted(uright, "gy", 1)
    ufrom_right = shifted(uleft, "gy", -1)
    back = pl.pallas_call(
        bind(adjoint_body),
        out_shape=plane(X),
        in_specs=[pl.BlockSpec(memory_space=pltpu.VMEM)] * 10,
        out_specs=pl.BlockSpec(memory_space=pltpu.VMEM),
        scratch_shapes=[pltpu.VMEM((X + 2 * H, L, LANES), F32)] * 2,
        name="adjoint",
    )(near, core, utop, ubot, ta, tb, top, bot, s, matst)
    bseam = call(
        bind(adjoint_seam_body), seam, (uleft, uright, ufrom_left, ufrom_right, coef, s, matst), "adjoint_seam")

    axes = ("tm", "gx", "gy")
    devices = lax.axis_size(axes)
    rdual, rincr, part = pl.pallas_call(
        bind(residual_body),
        out_shape=(sds(L * X, Y), sds(L * X, Y), sds(devices, LANES)),
        in_specs=[pl.BlockSpec(memory_space=pltpu.VMEM)] * 11,
        out_specs=(pl.BlockSpec(memory_space=pltpu.VMEM),) * 3,
        scratch_shapes=[pltpu.VMEM((L * X, Y), F32)] * 2,
        name="residual",
    )(ecore, enear, eseam, back, bseam, flat(forcing), flat(error_var), d, v, flat(gradient), flat(obs_weight))
    parts = lax.all_to_all(part, axes, 0, 0)
    count = 2 * increment.size * devices
    dnext, inext = call(
        functools.partial(update_body, count), (sds(L * X, Y), sds(L * X, Y)), (parts, d, v, rdual, rincr), "update")
    return dnext.reshape(increment.shape), inext.reshape(increment.shape)


def solution(mesh):
    field = P("tm", None, "gx", "gy")
    return jax.shard_map(
        local, mesh=mesh, in_specs=(field,) * 8 + (P(), P()), out_specs=(field, field), check_vma=False)
```

```python
import functools

import jax
import jax.numpy as jnp
from jax import lax
from jax.experimental import pallas as pl
from jax.experimental.pallas import tpu as pltpu
from jax.sharding import PartitionSpec as P


STEPS = 3
H = STEPS
LANES = 128
PITCH = 3 * H
F32 = jnp.float32
BF16 = jnp.bfloat16
VMEM_GRANT = 20 * 2**20
EDGES_GRANT = 52 * 2**20


def sds(*shape, dtype=F32):
    return jax.ShapeDtypeStruct(shape, dtype)


def call(body, outs, args, scratch=(), hbm=(), grant=VMEM_GRANT, outs_hbm=False):
    space = pl.BlockSpec(memory_space=pltpu.VMEM)
    outside = pl.BlockSpec(memory_space=pltpu.HBM)
    return pl.pallas_call(
        body,
        out_shape=outs,
        in_specs=[outside if i in hbm else space for i in range(len(args))],
        out_specs=jax.tree.map(lambda _: outside if outs_hbm else space, outs),
        scratch_shapes=list(scratch),
        compiler_params=pltpu.CompilerParams(vmem_limit_bytes=grant),
    )(*args)


def split(value):
    high = value.astype(BF16)
    return high, (value - high.astype(F32)).astype(BF16)


def mix(matrix, value):
    levels = value.shape[0]
    high, low = split(value)
    both = jnp.dot(matrix[...], high, preferred_element_type=F32)
    last = jnp.dot(matrix[0:levels, :], low, preferred_element_type=F32)
    return both[0:levels] + (both[levels:] + last)


def pairs(keys):
    keys = list(keys)
    return [keys[i : i + 2] for i in range(0, len(keys), 2)]


def mix_rows(matrix, rows):
    out = {}
    for group in pairs(sorted(rows)):
        wide = jnp.concatenate([rows[x] for x in group], axis=1) if len(group) > 1 else rows[group[0]]
        mixed = mix(matrix, wide)
        for place, x in enumerate(group):
            out[x] = mixed[:, place * LANES : (place + 1) * LANES]
    return out


def forward_row(v, a, b, s, x):
    here = v(x)
    out = (1.0 - a(x) - b(x) - 4.0 * s) * here
    out = out + (a(x - 1) + s) * v(x - 1) + s * v(x + 1)
    out = out + pltpu.roll((b(x) + s) * here, 1, 1)
    return out + s * pltpu.roll(here, LANES - 1, 1)


def adjoint_row(w, a, b, s, x):
    here = w(x)
    ax = a(x)
    bx = b(x)
    out = (1.0 - ax - bx - 4.0 * s) * here
    out = out + (ax + s) * w(x + 1) + s * w(x - 1)
    out = out + (bx + s) * pltpu.roll(here, LANES - 1, 1)
    return out + s * pltpu.roll(here, 1, 1)


def edge(axis, last):
    here = lax.axis_index(axis)
    return here == (lax.axis_size(axis) - 1 if last else 0)


def early():
    return lax.axis_index("tm") < lax.axis_size("tm") - 1


def late():
    return lax.axis_index("tm") > 0


def odd(axis):
    return lax.rem(lax.axis_index(axis), 2) == 1


def by_parity(axis, body):
    here = odd(axis)
    pl.when(here)(lambda: body(True))
    pl.when(jnp.logical_not(here))(lambda: body(False))


def only(condition, body):
    def run(*refs):
        pl.when(condition())(lambda: body(*refs))

    return run


def halo_fields(X, top, bot, tv, ta, tb, s):
    def v(x):
        return top[x + H] if x < 0 else (bot[x - X] if x >= X else tv[x])

    def a(x):
        if x == -H:
            return 1.0 - s
        return top[2 * H - 1 + x] if x < 0 else (bot[H + x - X] if x >= X else ta[x])

    def b(x):
        return top[3 * H - 2 + x] if x < 0 else (bot[2 * H - 1 + x - X] if x >= X else tb[x])

    return v, a, b


def landed(copies, ref, L):
    for copy in copies:
        copy.wait()
    pitch = ref.shape[1]
    return lambda x: ref.reshape(L * pitch, LANES)[pl.ds(x, L, stride=pitch), :]


def spans(size, parts, unit=1):
    step = -(-size // (parts * unit)) * unit
    return [(at, min(at + step, size)) for at in range(0, size, step)]


def landing_copies(pairs, X, sems):
    copies = []
    for i, (src, dst) in enumerate(pairs):
        own = []
        for j, (lo, hi) in enumerate(spans(src.shape[0], sems.shape[1])):
            own.append(pltpu.make_async_copy(src.at[lo:hi], dst.at[lo:hi, 0:X], sems.at[i, j]))
            own[-1].start()
        copies.append(own)
    return copies


def tight(ref, place, L):
    return ref.at[place * L : (place + 1) * L]


def loose(ref, place, L, LP):
    rows = tight(ref, place, L)[...]
    return jnp.concatenate([rows, jnp.zeros((LP - L, LANES), F32)], axis=0)


def put(rows, ref, place):
    L, LP = rows.shape[0], ref.shape[1]
    ref[place, 0:L] = rows
    ref[place, L:LP] = jnp.zeros((LP - L, LANES), F32)


def level_rows(diff, LP):
    L = diff.shape[1]
    rows = jnp.broadcast_to(diff[...], (LANES, L)).T
    return jnp.concatenate([rows, jnp.zeros((LP - L, LANES), F32)], axis=0)


def edges_body(X, L, v, a, b, d, diff, first, second, ufirst, usecond, vn, an, bn, dn, sems, sem):
    def fields(swapped):
        high, low = (second, first) if swapped else (first, second)
        small = pltpu.make_async_copy(diff, dn, sem)
        small.start()
        copies = landing_copies(((v, vn), (a, an), (b, bn)), X, sems)
        row_v = landed(copies[0], vn, L)
        for i in range(H):
            put(row_v(i), low, i)
            if i > 0:
                put(row_v(X - H + i), high, i)
        row_a = landed(copies[1], an, L)
        for i in range(H - 1):
            put(row_a(i), low, H + i)
            put(row_a(X - H + 1 + i), high, H + i)
        small.wait()
        put((row_a(X - H) + level_rows(dn, low.shape[1])[0:L]) * row_v(X - H), high, 0)
        row_b = landed(copies[2], bn, L)
        for i in range(H - 1):
            put(row_b(i), low, 2 * H - 1 + i)
            put(row_b(X - H + 1 + i), high, 2 * H - 1 + i)

    def dual(swapped):
        high, low = (usecond, ufirst) if swapped else (ufirst, usecond)
        copies = landing_copies(((d, vn),), X, sems)
        row = landed(copies[0], vn, L)
        for i in range(H):
            put(row(i), low, i)
            put(row(X - H + i), high, i)

    pl.when(early())(lambda: by_parity("gx", fields))
    pl.when(late())(lambda: by_parity("gx", dual))


LAG = 4


def wave(starts, ends):
    queues = [pairs(range(lo, hi)) for lo, hi in zip(starts, ends)]
    for i in range(max(LAG * step + len(queue) for step, queue in enumerate(queues))):
        for step, queue in enumerate(queues):
            if 0 <= i - LAG * step < len(queue):
                yield step, queue[i - LAG * step]


def core_body(X, L, v, a, b, m, diff, tv, ta, tb, mats, matst, sb, end, mid, one, two, vn, an, bn, sems):
    LP = tv.shape[1]
    copies = landing_copies(((v, vn), (a, an), (b, bn)), X, sems)
    for value, ref in ((m[...], mats), (m[...].T, matst)):
        ref[...] = jnp.zeros_like(ref)
        upper, lower = split(value)
        ref[0:L, 0:L] = upper
        ref[LP : LP + L, 0:L] = lower
    sb[...] = level_rows(diff, LP)
    readers = [landed(copy, src, L) for copy, src in zip(copies, (vn, an, bn))]
    done = [0]

    def put_to(limit):
        while done[0] < min(limit, X):
            for row, dst in zip(readers, (tv, ta, tb)):
                put(row(done[0]), dst, done[0])
            done[0] += 1

    s = sb[...]
    levels = [lambda x: tv[x], lambda x: one[x], lambda x: two[x]]
    for step, group in wave(range(1, H + 1), range(X - 1, X - 1 - H, -1)):
        if step == 0:
            put_to(group[-1] + 4)
        rows = {x: forward_row(levels[step], lambda x: ta[x], lambda x: tb[x], s, x) for x in group}
        for x, value in mix_rows(mats, rows).items():
            if step == 0:
                one[x] = value
            elif step == 1:
                two[x] = value
            else:
                tight(end, x - H, L)[...] = value[0:L]
    for place, (ref, x) in enumerate(
        ((one, 1), (one, 2), (one, X - 3), (one, X - 2), (two, 2), (two, 3), (two, X - 4), (two, X - 3))
    ):
        mid[place] = ref[x]


def fold_rows(value):
    return jnp.sum(value.reshape(-1, 8, LANES), axis=0)


def base_body(force, var, dual, incr, grad, obs, rd, ri, dk, ik, sums):
    d = dual[...]
    v = incr[...]
    for place, (ref, value) in enumerate(
        ((rd, force[...] - var[...] * d - v), (ri, grad[...] - obs[...] * v - d))
    ):
        ref[...] = value
        sums[place] = fold_rows(value * value)
    dk[...] = d
    ik[...] = v


def seam_add(field, rows, left, right):
    lane = lax.broadcasted_iota(jnp.int32, (1, LANES), 1)
    for r in rows:
        begin = PITCH * r
        rolled = pltpu.roll(field(r - H), (begin + 2 * H) % LANES, 1)
        for acc, offset in ((right, 0), (left, 2 * H)):
            for t in range(len(acc)):
                at = begin + offset - t * LANES
                if at < LANES and at + 2 * H > 0:
                    acc[t] = jnp.where((lane >= at) & (lane < at + 2 * H), rolled, acc[t])


def gather_own(X, field, left_ref, right_ref):
    LP = left_ref.shape[0]
    left = [jnp.zeros((LP, LANES), F32)] * 2
    right = [jnp.zeros((LP, LANES), F32)] * 2
    seam_add(field, range(H, X + H), left, right)
    for ref, value in ((left_ref, left), (right_ref, right)):
        ref[...] = jnp.concatenate(value, axis=1)


def padded_rows(X, L, LP, d):
    zeros = jnp.zeros((LP - L, LANES), F32)
    return lambda x: jnp.concatenate([d[pl.ds(x, L, stride=X), :], zeros], axis=0)


def gather_body(X, L, tv, ta, tb, d, own, uown):
    @pl.when(early())
    def _():
        for place, ref in enumerate((tv, ta, tb)):
            gather_own(X, lambda x: ref[x], own.at[2 * place], own.at[2 * place + 1])

    @pl.when(late())
    def _():
        gather_own(X, padded_rows(X, L, tv.shape[1], d), uown.at[0], uown.at[1])


def third(which):
    lane = lax.broadcasted_iota(jnp.int32, (1, 2 * LANES), 1)
    return lax.rem(lane, PITCH) // H == which


def roll(value, shift):
    return pltpu.roll(value, shift % value.shape[1], 1)


OUTER = tuple(range(H))


def assign(swapped, first, second, targets):
    below, above = (first, second) if swapped else (second, first)
    for source, (ref, start) in zip((below, above), targets):
        for i in range(source.shape[0]):
            ref[start + i] = source[i]


def ordered(axis, up, down):
    here = odd(axis)
    return jnp.where(here, down, up), jnp.where(here, up, down)


def upack_body(X, L, ufirst, usecond, own, uhalo, yfirst, ysecond, rows):
    by_parity("gx", lambda swapped: assign(swapped, ufirst, usecond, ((rows, 0), (rows, H))))
    for i in range(2 * H):
        tight(uhalo, i, L)[...] = rows[i, 0:L]
    left = [own[0, :, t * LANES : (t + 1) * LANES] for t in range(2)]
    right = [own[1, :, t * LANES : (t + 1) * LANES] for t in range(2)]
    places = OUTER + tuple(X + H + i for i in OUTER)
    seam_add(lambda x: rows[x + H] if x < 0 else rows[H + x - X], places, left, right)
    yfirst[...], ysecond[...] = ordered("gy", jnp.concatenate(right, axis=1), jnp.concatenate(left, axis=1))


def pack_body(X, first, second, own, sb, top, bot, full, yfirst, ysecond):
    by_parity("gx", lambda swapped: assign(swapped, first, second, ((top, 0), (bot, 0))))
    both = []
    for place, field in enumerate(halo_fields(X, top, bot, None, None, None, sb[...])):
        left = [own[2 * place, :, t * LANES : (t + 1) * LANES] for t in range(2)]
        right = [own[2 * place + 1, :, t * LANES : (t + 1) * LANES] for t in range(2)]
        rows = list(OUTER) + [X + H + i for i in OUTER]
        if place > 0:
            rows.remove(X + 2 * H - 1)
        if place > 1:
            rows.remove(0)
        seam_add(field, rows, left, right)
        left = jnp.concatenate(left, axis=1)
        right = jnp.concatenate(right, axis=1)
        full[2 * place] = left
        full[2 * place + 1] = right
        both.append((left, right))
    (lv, rv), (la, ra), (lb, rb) = both
    to_right = jnp.where(third(1), rv, jnp.where(third(2), roll(ra, H), roll(rb, 2 * H)))
    to_left = jnp.where(third(2), lv, jnp.where(third(0), roll(la, H), roll(lb, 2 * H)))
    yfirst[...], ysecond[...] = ordered("gy", to_right, to_left)


def rim_body(X, L, tv, ta, tb, top, bot, mid, sb, mats, out):
    s = sb[...]
    v, a, b = halo_fields(X, top, bot, tv, ta, tb, s)
    first = edge("gx", False)
    final = edge("gx", True)
    known = [
        {},
        {1: 0, 2: 1, X - 3: 2, X - 2: 3},
        {2: 4, 3: 5, X - 4: 6, X - 3: 7},
    ]
    state = None
    for step in range(H):
        got = state

        def current(x):
            if step == 0:
                return v(x)
            return mid[known[step][x]] if x in known[step] else got[x]

        reach = H - 1 - step
        rows = {}
        for x in list(range(-reach, H - reach)) + list(range(X - H + reach, X + reach)):
            rows[x] = forward_row(current, a, b, s, x)
        state = mix_rows(mats, rows)
        for x in state:
            if x < 0:
                state[x] = jnp.where(first, 0.0, state[x])
            if x >= X:
                state[x] = jnp.where(final, 0.0, state[x])
    for i in range(H):
        tight(out, i, L)[...] = state[i][0:L]
        tight(out, H + i, L)[...] = state[X - H + i][0:L]


def lanes_of_third(which, tile):
    return third(which)[:, tile * LANES : (tile + 1) * LANES]


def folds(X):
    begin = -(-(LANES - H) // PITCH) * PITCH - LANES
    half = (X + 2 * H - 1) * PITCH - LANES - begin
    return -(begin + H), half - (begin + 2 * H), half


def fold(X, left, right):
    first, second, half = folds(X)
    lane = lax.broadcasted_iota(jnp.int32, (1, LANES), 1)
    both = jnp.where(third(1), left, right)
    tail = both[:, LANES:]
    tail = jnp.where(lane < half, roll(tail, first), roll(tail, second))
    return jnp.where(lanes_of_third(0, 0), tail, both[:, :LANES])


def unfold(X, value):
    first, second, _ = folds(X)
    return value, jnp.where(lanes_of_third(1, 1), roll(value, -first), roll(value, -second))


def seam_masks(X):
    lane = lax.broadcasted_iota(jnp.int32, (1, 2 * LANES), 1)
    up, down = edge("gx", False), edge("gx", True)
    masks = []
    for shift, outer, where in ((H, "first", 1), (0, "last", 2)):
        out = (up & (lane < PITCH * H + shift)) | (down & (lane >= PITCH * (X + H) + shift))
        out = out | (edge("gy", outer == "last") & third(where))
        masks.append(jnp.where(out, 0.0, 1.0))
    return masks


def forward_seam(v, a, b, s, matrix):
    out = (1.0 - a - b - 4.0 * s) * v + s * (roll(v, -PITCH) + roll(v, -1))
    out = out + roll((a + s) * v, PITCH) + roll((b + s) * v, 1)
    return mix(matrix, out)


def adjoint_seam(u, a, b, s, matrix):
    w = mix(matrix, u)
    out = (1.0 - a - b - 4.0 * s) * w + s * (roll(w, PITCH) + roll(w, 1))
    return out + (a + s) * roll(w, -PITCH) + (b + s) * roll(w, -1)


def received(axis, first, second):
    here = odd(axis)
    first, second = first[...], second[...]
    return jnp.where(here, first, second), jnp.where(here, second, first)


def seam_body(X, full, yfirst, ysecond, uyfirst, uysecond, sb, mats, first, second, coef):
    def send(value, up):
        def body(swapped):
            ref = first if swapped != up else second
            ref[...] = value

        by_parity("tm", body)

    @pl.when(late())
    def _():
        send(fold(X, *received("gy", uyfirst, uysecond)), False)

    @pl.when(early())
    def _():
        one = sb[...]
        s = jnp.concatenate([one, one], axis=1)
        lo, hi = received("gy", yfirst, ysecond)
        lv = jnp.where(third(1), lo, full[0])
        rv = jnp.where(third(2), hi, full[1])
        coef[0] = jnp.where(third(1), roll(lo, -H), full[2])
        coef[1] = jnp.where(third(2), roll(hi, -H), full[3])
        coef[2] = jnp.where(third(1), roll(lo, -2 * H), full[4])
        coef[3] = jnp.where(third(2), roll(hi, -2 * H), full[5])
        left_in, right_in = seam_masks(X)
        for _ in range(H):
            lv = left_in * forward_seam(lv, coef[0], coef[2], s, mats)
            rv = right_in * forward_seam(rv, coef[1], coef[3], s, mats)
        send(fold(X, rv, lv), True)


def adjoint_core_body(X, L, d, ta, tb, sb, mats, out, mid, own, wide, state, dn, sems):
    s = sb[...]
    (copies,) = landing_copies(((d, dn),), X, sems)
    row = landed(copies, dn, L)
    for step, group in wave(range(H), range(X, X - H, -1)):
        base = step * X
        if step == 0:
            for x in group:
                put(row(x), state, x)
        for x, value in mix_rows(mats, {x: state[base + x] for x in group}).items():
            wide[base + x] = value
        for x in (group[0] - 1, group[0]):
            if step < x < X - step - 1:
                value = adjoint_row(lambda x: wide[base + x], lambda x: ta[x], lambda x: tb[x], s, x)
                if step == H - 1:
                    out[x - H] = value
                else:
                    state[base + X + x] = value
    for step in range(H):
        for place, x in enumerate((step, step + 1, X - 2 - step, X - 1 - step)):
            mid[4 * step + place] = wide[step * X + x]
    gather_own(X, lambda x: state[x], own.at[0], own.at[1])


def adjoint_rim_body(X, L, uhalo, mid, ta, tb, top, bot, sb, mats, brim):
    s = sb[...]
    _, a, b = halo_fields(X, top, bot, ta, ta, tb, s)
    first = edge("gx", False)
    final = edge("gx", True)
    LP = ta.shape[1]
    halo = {x: loose(uhalo, x + H, L, LP) for x in range(-H, 0)}
    halo.update({X + i: loose(uhalo, H + i, L, LP) for i in range(H)})
    state = halo
    for step in range(H):
        wide = mix_rows(mats, state)
        known = {x: 4 * step + i for i, x in enumerate((step, step + 1, X - 2 - step, X - 1 - step))}

        def current(x):
            return mid[known[x]] if x in known else wide[x]

        reach = H - 1 - step
        state = {}
        for x in list(range(-reach, H - reach)) + list(range(X - H + reach, X + reach)):
            value = adjoint_row(current, a, b, s, x)
            if x < 0:
                value = jnp.where(first, 0.0, value)
            if x >= X:
                value = jnp.where(final, 0.0, value)
            state[x] = value
    for i in range(H):
        brim[i] = state[i]
        brim[H + i] = state[X - H + i]


def adjoint_seam_body(X, L, uhalo, tfirst, tsecond, own, coef, sb, mats, bseam):
    s = sb[...]
    LP = s.shape[0]
    halo = {x: loose(uhalo, x + H, L, LP) for x in range(-H, 0)}
    halo.update({X + i: loose(uhalo, H + i, L, LP) for i in range(H)})
    s = jnp.concatenate([s, s], axis=1)
    left = [own[0, :, t * LANES : (t + 1) * LANES] for t in range(2)]
    right = [own[1, :, t * LANES : (t + 1) * LANES] for t in range(2)]
    seam_add(lambda x: halo[x], list(range(H)) + list(range(X + H, X + 2 * H)), left, right)
    _, useam = received("tm", tfirst, tsecond)
    outer = jnp.concatenate(unfold(X, useam), axis=1)
    lu = jnp.where(third(1), outer, jnp.concatenate(left, axis=1))
    ru = jnp.where(third(2), outer, jnp.concatenate(right, axis=1))
    left_in, right_in = seam_masks(X)
    for _ in range(H):
        lu = left_in * adjoint_seam(lu, coef[0], coef[2], s, mats)
        ru = right_in * adjoint_seam(ru, coef[1], coef[3], s, mats)
    bseam[...] = fold(X, ru, lu)


def merged_row(X, L, core, rim, seam, x):
    ref, place = (core, x - H) if H <= x < X - H else (rim, x if x < H else x - X + 2 * H)
    row = ref[place, 0:L] if len(ref.shape) == 3 else tight(ref, place, L)[...]
    at = PITCH * (x + H) + H
    lane = lax.broadcasted_iota(jnp.int32, (1, LANES), 1)
    rolled = pltpu.roll(seam[at // LANES], (LANES - H - at) % LANES, 1)
    return jnp.where((lane < H) | (lane >= LANES - H), rolled, row)


def residual_body(X, L, ecore, erim, tfirst, tsecond, bcore, brim, bseam, rd, ri, sums, rdual, rincr, part, total):
    for index, (changes, core, rim, seam, base, out) in enumerate(
        ((late(), ecore, erim, None, rd, rdual), (early(), bcore, brim, bseam, ri, rincr))
    ):

        @pl.when(changes)
        def _():
            value = received("tm", tfirst, tsecond)[0] if seam is None else seam[...]
            tiles = unfold(X, value[0:L])
            squares = jnp.zeros((1, LANES), F32)
            for x in range(X):
                place = pl.ds(x, L, stride=X)
                value = base[place, :] + merged_row(X, L, core, rim, tiles, x)
                out[place, :] = value
                squares = squares + jnp.sum(value * value, axis=0, keepdims=True)
            total[index] = squares

        @pl.when(jnp.logical_not(changes))
        def _():
            out[...] = base[...]
            total[index] = jnp.sum(sums[index], axis=0, keepdims=True)

    part[...] = jnp.broadcast_to(jnp.sum(total[0] + total[1], keepdims=True), part.shape)


def update_body(count, parts, dual, incr, rdual, rincr, dnext, inext, made, sems):
    total = jnp.sum(parts[:, 0:1], keepdims=True)
    scale = jnp.minimum(1.0, 0.5 / jnp.sqrt(total * (1.0 / count) + 1e-06))
    copies = []
    for j, (lo, hi) in enumerate(spans(dual.shape[0], sems.shape[1], 8)):
        for i, (old, change, new) in enumerate(((dual, rdual, dnext), (incr, rincr, inext))):
            made[i, lo:hi] = old[lo:hi] + scale * change[lo:hi]
            copies.append(pltpu.make_async_copy(made.at[i, lo:hi], new.at[lo:hi], sems.at[i, j]))
            copies[-1].start()
    for copy in copies:
        copy.wait()


def shifted(block, axis, distance):
    count = lax.axis_size(axis)
    return lax.ppermute(block, axis, [(i - distance, i) for i in range(count) if 0 <= i - distance < count])


def local(increment, dual_state, forcing, gradient, courant_x, courant_y, error_var, obs_weight, diffusion, level_mix):
    _, L, X, Y = increment.shape
    assert Y == LANES and X % 8 == 0 and X > 2 * H and PITCH * (X + 2 * H) + 2 * H <= 2 * LANES
    LP = -(-L // 16) * 16
    flat = lambda t: t.reshape(L * X, Y)
    block = lambda t: t.reshape(L, X, Y)
    v, d = flat(increment), flat(dual_state)
    plane = lambda n: sds(n, LP, LANES)
    wide = lambda n: sds(n, LP, 2 * LANES)
    packed = lambda n: sds(n * L, LANES)
    natural = sds(L * X, Y)
    single = sds(LP, LANES)
    seam = sds(LP, 2 * LANES)
    matrix = sds(2 * LP, LP, dtype=BF16)
    scratch = lambda n: pltpu.VMEM((n, LP, LANES), F32)
    bind = lambda body, *sizes: functools.partial(body, *sizes)
    windows = lax.axis_size("tm")
    forward, backward = range(windows - 1), range(1, windows)

    dual_later = shifted(dual_state, "tm", -1)
    landing = [pltpu.VMEM((L, X + 8, LANES), F32)] * 3 + [pltpu.SemaphoreType.DMA((3, 4))]
    fields = (block(increment), block(courant_x), block(courant_y))
    rows = call(
        bind(edges_body, X, L), (plane(3 * H - 2), plane(3 * H - 2), plane(H), plane(H)),
        fields + (block(dual_state), diffusion[None, :]),
        landing[:3] + [pltpu.VMEM((1, L), F32)] + landing[3:] + [pltpu.SemaphoreType.DMA],
        hbm=range(5), grant=EDGES_GRANT)
    halo = exchange(rows[0], rows[1], "gx", forward)
    uhalo = exchange(rows[2], rows[3], "gx", backward)
    tv, ta, tb, mats, matst, sb, ecore, mid = call(
        only(early, bind(core_body, X, L)),
        (plane(X),) * 3 + (matrix, matrix, single, packed(X - 2 * H), plane(8)),
        fields + (level_mix, diffusion[None, :]), [scratch(X), scratch(X)] + landing, hbm=range(3))
    ecore = shifted(ecore, "tm", 1)
    own, uown = call(bind(gather_body, X, L), (wide(6), wide(2)), (tv, ta, tb, d))
    uhalo, uyfirst, uysecond = call(
        only(late, bind(upack_body, X, L)), (packed(2 * H), seam, seam), (*uhalo, uown), [scratch(2 * H)])
    uhalo = shifted(uhalo, "tm", -1)
    ufrom = exchange(uyfirst, uysecond, "gy", backward)
    rd, ri, dk, ik, sums = call(
        base_body, (natural,) * 4 + (sds(2, 8, LANES),),
        (flat(forcing), flat(error_var), d, v, flat(gradient), flat(obs_weight)))

    top, bot, full, yfirst, ysecond = call(
        only(early, bind(pack_body, X)),
        (plane(3 * H - 2), plane(3 * H - 2), wide(6), seam, seam), (*halo, own, sb))
    sides = exchange(yfirst, ysecond, "gy", forward)
    erim = call(
        only(early, bind(rim_body, X, L)), packed(2 * H), (tv, ta, tb, top, bot, mid, sb, mats))
    erim = shifted(erim, "tm", 1)
    tfirst, tsecond, coef = call(
        bind(seam_body, X), (single, single, wide(4)), (full, *sides, *ufrom, sb, mats))
    seams = exchange(tfirst, tsecond, "tm")

    bcore, bmid, dual_own = call(
        only(early, bind(adjoint_core_body, X, L)),
        (plane(X - 2 * H), plane(4 * H), wide(2)),
        (block(dual_later), ta, tb, sb, matst), [scratch(H * X), scratch(H * X), landing[0], landing[3]],
        hbm=(0,))
    brim = call(
        only(early, bind(adjoint_rim_body, X, L)), plane(2 * H), (uhalo, bmid, ta, tb, top, bot, sb, matst))
    bseam = call(
        only(early, bind(adjoint_seam_body, X, L)), single, (uhalo, *seams, dual_own, coef, sb, matst))

    axes = ("tm", "gx", "gy")
    devices = lax.axis_size(axes)
    rdual, rincr, part = call(
        bind(residual_body, X, L), (natural, natural, sds(devices, LANES)),
        (ecore, erim, *seams, bcore, brim, bseam, rd, ri, sums), [pltpu.VMEM((2, 1, LANES), F32)])
    parts = lax.all_to_all(part, axes, 0, 0)
    count = 2 * increment.size * devices
    dnext, inext = call(
        bind(update_body, count), (natural, natural), (parts, dk, ik, rdual, rincr),
        [pltpu.VMEM((2, L * X, Y), F32), pltpu.SemaphoreType.DMA((2, 4))], outs_hbm=True)
    return dnext.reshape(increment.shape), inext.reshape(increment.shape)


def exchange(first, second, axis, windows=None):
    count = lax.axis_size(axis)
    out = []
    for turn, block in enumerate((first, second)):
        starts = range(turn, count - 1, 2)
        route = [pair for i in starts for pair in ((i, i + 1), (i + 1, i))]
        if not route:
            out.append(out[0])
            continue
        if windows is None:
            out.append(lax.ppermute(block, axis, route))
        else:
            wide = [(w * count + i, w * count + j) for w in windows for i, j in route]
            out.append(lax.ppermute(block, ("tm", axis), wide))
    return out


def solution(mesh):
    field = P("tm", None, "gx", "gy")
    return jax.shard_map(
        local, mesh=mesh, in_specs=(field,) * 8 + (P(), P()), out_specs=(field, field), check_vma=False)
```

```python
import functools

import jax
import jax.numpy as jnp
from jax import lax
from jax.experimental import pallas as pl
from jax.experimental.pallas import tpu as pltpu
from jax.sharding import PartitionSpec as P


STEPS = 3
H = STEPS
LANES = 128
PITCH = 3 * H
F32 = jnp.float32
BF16 = jnp.bfloat16
VMEM_GRANT = 20 * 2**20
EDGES_GRANT = 52 * 2**20
START_FLOPS = 10**9


def sds(*shape, dtype=F32):
    return jax.ShapeDtypeStruct(shape, dtype)


def call(body, outs, args, scratch=(), hbm=(), grant=VMEM_GRANT, outs_hbm=False, flops=None):
    space = pl.BlockSpec(memory_space=pltpu.VMEM)
    outside = pl.BlockSpec(memory_space=pltpu.HBM)
    return pl.pallas_call(
        body,
        out_shape=outs,
        in_specs=[outside if i in hbm else space for i in range(len(args))],
        out_specs=jax.tree.map(lambda _: outside if outs_hbm else space, outs),
        scratch_shapes=list(scratch),
        compiler_params=pltpu.CompilerParams(vmem_limit_bytes=grant),
        cost_estimate=None if flops is None else pl.CostEstimate(flops=flops, bytes_accessed=0, transcendentals=0),
    )(*args)


def split(value):
    high = value.astype(BF16)
    return high, (value - high.astype(F32)).astype(BF16)


def mix(matrix, value):
    levels = value.shape[0]
    high, low = split(value)
    both = jnp.dot(matrix[...], high, preferred_element_type=F32)
    last = jnp.dot(matrix[0:levels, :], low, preferred_element_type=F32)
    return both[0:levels] + (both[levels:] + last)


def pairs(keys):
    keys = list(keys)
    return [keys[i : i + 2] for i in range(0, len(keys), 2)]


def mix_rows(matrix, rows):
    out = {}
    for group in pairs(sorted(rows)):
        wide = jnp.concatenate([rows[x] for x in group], axis=1) if len(group) > 1 else rows[group[0]]
        mixed = mix(matrix, wide)
        for place, x in enumerate(group):
            out[x] = mixed[:, place * LANES : (place + 1) * LANES]
    return out


def forward_row(v, a, b, s, x):
    here = v(x)
    out = (1.0 - a(x) - b(x) - 4.0 * s) * here
    out = out + (a(x - 1) + s) * v(x - 1) + s * v(x + 1)
    out = out + pltpu.roll((b(x) + s) * here, 1, 1)
    return out + s * pltpu.roll(here, LANES - 1, 1)


def adjoint_row(w, a, b, s, x):
    here = w(x)
    ax = a(x)
    bx = b(x)
    out = (1.0 - ax - bx - 4.0 * s) * here
    out = out + (ax + s) * w(x + 1) + s * w(x - 1)
    out = out + (bx + s) * pltpu.roll(here, LANES - 1, 1)
    return out + s * pltpu.roll(here, 1, 1)


def edge(axis, last):
    here = lax.axis_index(axis)
    return here == (lax.axis_size(axis) - 1 if last else 0)


def early():
    return lax.axis_index("tm") < lax.axis_size("tm") - 1


def late():
    return lax.axis_index("tm") > 0


def odd(axis):
    return lax.rem(lax.axis_index(axis), 2) == 1


def by_parity(axis, body):
    here = odd(axis)
    pl.when(here)(lambda: body(True))
    pl.when(jnp.logical_not(here))(lambda: body(False))


def only(condition, body):
    def run(*refs):
        pl.when(condition())(lambda: body(*refs))

    return run


def halo_fields(X, top, bot, tv, ta, tb, s):
    def v(x):
        return top[x + H] if x < 0 else (bot[x - X] if x >= X else tv[x])

    def a(x):
        if x == -H:
            return 1.0 - s
        return top[2 * H - 1 + x] if x < 0 else (bot[H + x - X] if x >= X else ta[x])

    def b(x):
        return top[3 * H - 2 + x] if x < 0 else (bot[2 * H - 1 + x - X] if x >= X else tb[x])

    return v, a, b


def landed(copies, ref, L):
    for copy in copies:
        copy.wait()
    pitch = ref.shape[1]
    return lambda x: ref.reshape(L * pitch, LANES)[pl.ds(x, L, stride=pitch), :]


def spans(size, parts, unit=1):
    step = -(-size // (parts * unit)) * unit
    return [(at, min(at + step, size)) for at in range(0, size, step)]


def landing_copies(pairs, X, sems):
    copies = []
    for i, (src, dst) in enumerate(pairs):
        own = []
        for j, (lo, hi) in enumerate(spans(src.shape[0], sems.shape[1])):
            own.append(pltpu.make_async_copy(src.at[lo:hi], dst.at[lo:hi, 0:X], sems.at[i, j]))
            own[-1].start()
        copies.append(own)
    return copies


def tight(ref, place, L):
    return ref.at[place * L : (place + 1) * L]


def loose(ref, place, L, LP):
    rows = tight(ref, place, L)[...]
    return jnp.concatenate([rows, jnp.zeros((LP - L, LANES), F32)], axis=0)


def put(rows, ref, place):
    L, LP = rows.shape[0], ref.shape[1]
    ref[place, 0:L] = rows
    ref[place, L:LP] = jnp.zeros((LP - L, LANES), F32)


def level_rows(diff, LP):
    L = diff.shape[1]
    rows = jnp.broadcast_to(diff[...], (LANES, L)).T
    return jnp.concatenate([rows, jnp.zeros((LP - L, LANES), F32)], axis=0)


def start_body(out):
    out[...] = jnp.zeros_like(out)


def edges_body(X, L, v, a, b, d, diff, _, first, second, ufirst, usecond, vn, an, bn, dn, sems, sem):
    def fields(swapped):
        high, low = (second, first) if swapped else (first, second)
        small = pltpu.make_async_copy(diff, dn, sem)
        small.start()
        copies = landing_copies(((v, vn), (a, an), (b, bn)), X, sems)
        row_v = landed(copies[0], vn, L)
        for i in range(H):
            tight(low, i, L)[...] = row_v(i)
            if i > 0:
                tight(high, i, L)[...] = row_v(X - H + i)
        row_a = landed(copies[1], an, L)
        for i in range(H - 1):
            tight(low, H + i, L)[...] = row_a(i)
            tight(high, H + i, L)[...] = row_a(X - H + 1 + i)
        small.wait()
        tight(high, 0, L)[...] = (row_a(X - H) + level_rows(dn, ufirst.shape[1])[0:L]) * row_v(X - H)
        row_b = landed(copies[2], bn, L)
        for i in range(H - 1):
            tight(low, 2 * H - 1 + i, L)[...] = row_b(i)
            tight(high, 2 * H - 1 + i, L)[...] = row_b(X - H + 1 + i)

    def dual(swapped):
        high, low = (usecond, ufirst) if swapped else (ufirst, usecond)
        copies = landing_copies(((d, vn),), X, sems)
        row = landed(copies[0], vn, L)
        for i in range(H):
            put(row(i), low, i)
            put(row(X - H + i), high, i)

    pl.when(early())(lambda: by_parity("gx", fields))
    pl.when(late())(lambda: by_parity("gx", dual))


LAG = 4


def wave(starts, ends):
    queues = [pairs(range(lo, hi)) for lo, hi in zip(starts, ends)]
    for i in range(max(LAG * step + len(queue) for step, queue in enumerate(queues))):
        for step, queue in enumerate(queues):
            if 0 <= i - LAG * step < len(queue):
                yield step, queue[i - LAG * step]


def core_body(X, L, v, a, b, m, diff, tv, ta, tb, mats, matst, sb, end, mid, one, two, vn, an, bn, sems):
    LP = tv.shape[1]
    blocks = ((v, vn), (a, an), (b, bn))
    halves = spans(X, 2, 8)
    waiting = []
    for part, (lo, hi) in enumerate(halves):
        for i, (src, dst) in enumerate(blocks):
            for j, (low, high) in enumerate(spans(L, sems.shape[1] // 2)):
                copy = pltpu.make_async_copy(
                    src.at[low:high, lo:hi], dst.at[low:high, lo:hi], sems.at[i, 2 * part + j])
                copy.start()
                waiting.append((lo, copy))
    for value, ref in ((m[...], mats), (m[...].T, matst)):
        ref[...] = jnp.zeros_like(ref)
        upper, lower = split(value)
        ref[0:L, 0:L] = upper
        ref[LP : LP + L, 0:L] = lower
    sb[...] = level_rows(diff, LP)
    readers = [landed((), src, L) for src in (vn, an, bn)]
    done = [0]

    def put_to(limit):
        while done[0] < min(limit, X):
            while waiting and waiting[0][0] <= done[0]:
                waiting.pop(0)[1].wait()
            for row, dst in zip(readers, (tv, ta, tb)):
                put(row(done[0]), dst, done[0])
            done[0] += 1

    s = sb[...]
    levels = [lambda x: tv[x], lambda x: one[x], lambda x: two[x]]
    for step, group in wave(range(1, H + 1), range(X - 1, X - 1 - H, -1)):
        if step == 0:
            put_to(group[-1] + 4)
        rows = {x: forward_row(levels[step], lambda x: ta[x], lambda x: tb[x], s, x) for x in group}
        for x, value in mix_rows(mats, rows).items():
            if step == 0:
                one[x] = value
            elif step == 1:
                two[x] = value
            else:
                tight(end, x - H, L)[...] = value[0:L]
    for place, (ref, x) in enumerate(
        ((one, 1), (one, 2), (one, X - 3), (one, X - 2), (two, 2), (two, 3), (two, X - 4), (two, X - 3))
    ):
        mid[place] = ref[x]


def fold_rows(value):
    return jnp.sum(value.reshape(-1, 8, LANES), axis=0)


def base_body(force, var, dual, incr, grad, obs, rd, ri, dk, ik, sums):
    d = dual[...]
    v = incr[...]
    for place, (ref, value) in enumerate(
        ((rd, force[...] - var[...] * d - v), (ri, grad[...] - obs[...] * v - d))
    ):
        ref[...] = value
        sums[place] = fold_rows(value * value)
    dk[...] = d
    ik[...] = v


def seam_add(field, rows, left, right):
    lane = lax.broadcasted_iota(jnp.int32, (1, LANES), 1)
    for r in rows:
        begin = PITCH * r
        rolled = pltpu.roll(field(r - H), (begin + 2 * H) % LANES, 1)
        for acc, offset in ((right, 0), (left, 2 * H)):
            for t in range(len(acc)):
                at = begin + offset - t * LANES
                if at < LANES and at + 2 * H > 0:
                    acc[t] = jnp.where((lane >= at) & (lane < at + 2 * H), rolled, acc[t])


def gather_own(X, field, left_ref, right_ref):
    LP = left_ref.shape[0]
    left = [jnp.zeros((LP, LANES), F32)] * 2
    right = [jnp.zeros((LP, LANES), F32)] * 2
    seam_add(field, range(H, X + H), left, right)
    for ref, value in ((left_ref, left), (right_ref, right)):
        ref[...] = jnp.concatenate(value, axis=1)


def padded_rows(X, L, LP, d):
    zeros = jnp.zeros((LP - L, LANES), F32)
    return lambda x: jnp.concatenate([d[pl.ds(x, L, stride=X), :], zeros], axis=0)


def gather_body(X, L, tv, ta, tb, d, own, uown):
    @pl.when(early())
    def _():
        for place, ref in enumerate((tv, ta, tb)):
            gather_own(X, lambda x: ref[x], own.at[2 * place], own.at[2 * place + 1])

    @pl.when(late())
    def _():
        gather_own(X, padded_rows(X, L, tv.shape[1], d), uown.at[0], uown.at[1])


def third(which):
    lane = lax.broadcasted_iota(jnp.int32, (1, 2 * LANES), 1)
    return lax.rem(lane, PITCH) // H == which


def roll(value, shift):
    return pltpu.roll(value, shift % value.shape[1], 1)


OUTER = tuple(range(H))


def assign(swapped, first, second, targets):
    below, above = (first, second) if swapped else (second, first)
    for source, (ref, start) in zip((below, above), targets):
        if len(source.shape) == 3:
            for i in range(source.shape[0]):
                ref[start + i] = source[i]
        else:
            L = source.shape[0] // ref.shape[0]
            for i in range(ref.shape[0]):
                ref[i] = loose(source, i, L, ref.shape[1])


def ordered(axis, up, down):
    here = odd(axis)
    return jnp.where(here, down, up), jnp.where(here, up, down)


def upack_body(X, L, ufirst, usecond, own, uhalo, yfirst, ysecond, rows):
    by_parity("gx", lambda swapped: assign(swapped, ufirst, usecond, ((rows, 0), (rows, H))))
    for i in range(2 * H):
        tight(uhalo, i, L)[...] = rows[i, 0:L]
    left = [own[0, :, t * LANES : (t + 1) * LANES] for t in range(2)]
    right = [own[1, :, t * LANES : (t + 1) * LANES] for t in range(2)]
    places = OUTER + tuple(X + H + i for i in OUTER)
    seam_add(lambda x: rows[x + H] if x < 0 else rows[H + x - X], places, left, right)
    yfirst[...], ysecond[...] = ordered("gy", jnp.concatenate(right, axis=1), jnp.concatenate(left, axis=1))


def pack_body(X, first, second, own, sb, top, bot, full, yfirst, ysecond):
    by_parity("gx", lambda swapped: assign(swapped, first, second, ((top, 0), (bot, 0))))
    both = []
    for place, field in enumerate(halo_fields(X, top, bot, None, None, None, sb[...])):
        left = [own[2 * place, :, t * LANES : (t + 1) * LANES] for t in range(2)]
        right = [own[2 * place + 1, :, t * LANES : (t + 1) * LANES] for t in range(2)]
        rows = list(OUTER) + [X + H + i for i in OUTER]
        if place > 0:
            rows.remove(X + 2 * H - 1)
        if place > 1:
            rows.remove(0)
        seam_add(field, rows, left, right)
        left = jnp.concatenate(left, axis=1)
        right = jnp.concatenate(right, axis=1)
        full[2 * place] = left
        full[2 * place + 1] = right
        both.append((left, right))
    (lv, rv), (la, ra), (lb, rb) = both
    to_right = jnp.where(third(1), rv, jnp.where(third(2), roll(ra, H), roll(rb, 2 * H)))
    to_left = jnp.where(third(2), lv, jnp.where(third(0), roll(la, H), roll(lb, 2 * H)))
    yfirst[...], ysecond[...] = ordered("gy", to_right, to_left)


def rim_body(X, L, tv, ta, tb, top, bot, mid, sb, mats, out):
    s = sb[...]
    v, a, b = halo_fields(X, top, bot, tv, ta, tb, s)
    first = edge("gx", False)
    final = edge("gx", True)
    known = [
        {},
        {1: 0, 2: 1, X - 3: 2, X - 2: 3},
        {2: 4, 3: 5, X - 4: 6, X - 3: 7},
    ]
    state = None
    for step in range(H):
        got = state

        def current(x):
            if step == 0:
                return v(x)
            return mid[known[step][x]] if x in known[step] else got[x]

        reach = H - 1 - step
        rows = {}
        for x in list(range(-reach, H - reach)) + list(range(X - H + reach, X + reach)):
            rows[x] = forward_row(current, a, b, s, x)
        state = mix_rows(mats, rows)
        for x in state:
            if x < 0:
                state[x] = jnp.where(first, 0.0, state[x])
            if x >= X:
                state[x] = jnp.where(final, 0.0, state[x])
    for i in range(H):
        tight(out, i, L)[...] = state[i][0:L]
        tight(out, H + i, L)[...] = state[X - H + i][0:L]


def lanes_of_third(which, tile):
    return third(which)[:, tile * LANES : (tile + 1) * LANES]


def folds(X):
    begin = -(-(LANES - H) // PITCH) * PITCH - LANES
    half = (X + 2 * H - 1) * PITCH - LANES - begin
    return -(begin + H), half - (begin + 2 * H), half


def fold(X, left, right):
    first, second, half = folds(X)
    lane = lax.broadcasted_iota(jnp.int32, (1, LANES), 1)
    both = jnp.where(third(1), left, right)
    tail = both[:, LANES:]
    tail = jnp.where(lane < half, roll(tail, first), roll(tail, second))
    return jnp.where(lanes_of_third(0, 0), tail, both[:, :LANES])


def unfold(X, value):
    first, second, _ = folds(X)
    return value, jnp.where(lanes_of_third(1, 1), roll(value, -first), roll(value, -second))


def seam_masks(X):
    lane = lax.broadcasted_iota(jnp.int32, (1, 2 * LANES), 1)
    up, down = edge("gx", False), edge("gx", True)
    masks = []
    for shift, outer, where in ((H, "first", 1), (0, "last", 2)):
        out = (up & (lane < PITCH * H + shift)) | (down & (lane >= PITCH * (X + H) + shift))
        out = out | (edge("gy", outer == "last") & third(where))
        masks.append(jnp.where(out, 0.0, 1.0))
    return masks


def forward_seam(v, a, b, s, matrix):
    out = (1.0 - a - b - 4.0 * s) * v + s * (roll(v, -PITCH) + roll(v, -1))
    out = out + roll((a + s) * v, PITCH) + roll((b + s) * v, 1)
    return mix(matrix, out)


def adjoint_seam(u, a, b, s, matrix):
    w = mix(matrix, u)
    out = (1.0 - a - b - 4.0 * s) * w + s * (roll(w, PITCH) + roll(w, 1))
    return out + (a + s) * roll(w, -PITCH) + (b + s) * roll(w, -1)


def received(axis, first, second):
    here = odd(axis)
    first, second = first[...], second[...]
    return jnp.where(here, first, second), jnp.where(here, second, first)


def seam_body(X, full, yfirst, ysecond, uyfirst, uysecond, sb, mats, first, second, coef):
    def send(value, up):
        def body(swapped):
            ref = first if swapped != up else second
            ref[...] = value

        by_parity("tm", body)

    @pl.when(late())
    def _():
        send(fold(X, *received("gy", uyfirst, uysecond)), False)

    @pl.when(early())
    def _():
        one = sb[...]
        s = jnp.concatenate([one, one], axis=1)
        lo, hi = received("gy", yfirst, ysecond)
        lv = jnp.where(third(1), lo, full[0])
        rv = jnp.where(third(2), hi, full[1])
        coef[0] = jnp.where(third(1), roll(lo, -H), full[2])
        coef[1] = jnp.where(third(2), roll(hi, -H), full[3])
        coef[2] = jnp.where(third(1), roll(lo, -2 * H), full[4])
        coef[3] = jnp.where(third(2), roll(hi, -2 * H), full[5])
        left_in, right_in = seam_masks(X)
        for _ in range(H):
            lv = left_in * forward_seam(lv, coef[0], coef[2], s, mats)
            rv = right_in * forward_seam(rv, coef[1], coef[3], s, mats)
        send(fold(X, rv, lv), True)


def adjoint_core_body(X, L, d, ta, tb, sb, mats, out, mid, own, wide, state, dn, sems):
    s = sb[...]
    (copies,) = landing_copies(((d, dn),), X, sems)
    row = landed(copies, dn, L)
    for step, group in wave(range(H), range(X, X - H, -1)):
        base = step * X
        if step == 0:
            for x in group:
                put(row(x), state, x)
        for x, value in mix_rows(mats, {x: state[base + x] for x in group}).items():
            wide[base + x] = value
        for x in (group[0] - 1, group[0]):
            if step < x < X - step - 1:
                value = adjoint_row(lambda x: wide[base + x], lambda x: ta[x], lambda x: tb[x], s, x)
                if step == H - 1:
                    out[x - H] = value
                else:
                    state[base + X + x] = value
    for step in range(H):
        for place, x in enumerate((step, step + 1, X - 2 - step, X - 1 - step)):
            mid[4 * step + place] = wide[step * X + x]
    gather_own(X, lambda x: state[x], own.at[0], own.at[1])


def adjoint_rim_body(X, L, uhalo, mid, ta, tb, top, bot, sb, mats, brim):
    s = sb[...]
    _, a, b = halo_fields(X, top, bot, ta, ta, tb, s)
    first = edge("gx", False)
    final = edge("gx", True)
    LP = ta.shape[1]
    halo = {x: loose(uhalo, x + H, L, LP) for x in range(-H, 0)}
    halo.update({X + i: loose(uhalo, H + i, L, LP) for i in range(H)})
    state = halo
    for step in range(H):
        wide = mix_rows(mats, state)
        known = {x: 4 * step + i for i, x in enumerate((step, step + 1, X - 2 - step, X - 1 - step))}

        def current(x):
            return mid[known[x]] if x in known else wide[x]

        reach = H - 1 - step
        state = {}
        for x in list(range(-reach, H - reach)) + list(range(X - H + reach, X + reach)):
            value = adjoint_row(current, a, b, s, x)
            if x < 0:
                value = jnp.where(first, 0.0, value)
            if x >= X:
                value = jnp.where(final, 0.0, value)
            state[x] = value
    for i in range(H):
        brim[i] = state[i]
        brim[H + i] = state[X - H + i]


def adjoint_seam_body(X, L, uhalo, tfirst, tsecond, own, coef, sb, mats, bseam):
    s = sb[...]
    LP = s.shape[0]
    halo = {x: loose(uhalo, x + H, L, LP) for x in range(-H, 0)}
    halo.update({X + i: loose(uhalo, H + i, L, LP) for i in range(H)})
    s = jnp.concatenate([s, s], axis=1)
    left = [own[0, :, t * LANES : (t + 1) * LANES] for t in range(2)]
    right = [own[1, :, t * LANES : (t + 1) * LANES] for t in range(2)]
    seam_add(lambda x: halo[x], list(range(H)) + list(range(X + H, X + 2 * H)), left, right)
    _, useam = received("tm", tfirst, tsecond)
    outer = jnp.concatenate(unfold(X, useam), axis=1)
    lu = jnp.where(third(1), outer, jnp.concatenate(left, axis=1))
    ru = jnp.where(third(2), outer, jnp.concatenate(right, axis=1))
    left_in, right_in = seam_masks(X)
    for _ in range(H):
        lu = left_in * adjoint_seam(lu, coef[0], coef[2], s, mats)
        ru = right_in * adjoint_seam(ru, coef[1], coef[3], s, mats)
    bseam[...] = fold(X, ru, lu)


def merged_row(X, L, core, rim, seam, x):
    ref, place = (core, x - H) if H <= x < X - H else (rim, x if x < H else x - X + 2 * H)
    row = ref[place, 0:L] if len(ref.shape) == 3 else tight(ref, place, L)[...]
    at = PITCH * (x + H) + H
    lane = lax.broadcasted_iota(jnp.int32, (1, LANES), 1)
    rolled = pltpu.roll(seam[at // LANES], (LANES - H - at) % LANES, 1)
    return jnp.where((lane < H) | (lane >= LANES - H), rolled, row)


def residual_body(X, L, ecore, erim, tfirst, tsecond, bcore, brim, bseam, rd, ri, sums, rdual, rincr, part, total):
    for index, (changes, core, rim, seam, base, out) in enumerate(
        ((late(), ecore, erim, None, rd, rdual), (early(), bcore, brim, bseam, ri, rincr))
    ):

        @pl.when(changes)
        def _():
            value = received("tm", tfirst, tsecond)[0] if seam is None else seam[...]
            tiles = unfold(X, value[0:L])
            squares = jnp.zeros((1, LANES), F32)
            for x in range(X):
                place = pl.ds(x, L, stride=X)
                value = base[place, :] + merged_row(X, L, core, rim, tiles, x)
                out[place, :] = value
                squares = squares + jnp.sum(value * value, axis=0, keepdims=True)
            total[index] = squares

        @pl.when(jnp.logical_not(changes))
        def _():
            out[...] = base[...]
            total[index] = jnp.sum(sums[index], axis=0, keepdims=True)

    part[...] = jnp.broadcast_to(jnp.sum(total[0] + total[1], keepdims=True), part.shape)


def update_body(count, parts, dual, incr, rdual, rincr, dnext, inext, made, sems):
    total = jnp.sum(parts[:, 0:1], keepdims=True)
    scale = jnp.minimum(1.0, 0.5 / jnp.sqrt(total * (1.0 / count) + 1e-06))
    copies = []
    for j, (lo, hi) in enumerate(spans(dual.shape[0], sems.shape[1], 8)):
        for i, (old, change, new) in enumerate(((dual, rdual, dnext), (incr, rincr, inext))):
            made[i, lo:hi] = old[lo:hi] + scale * change[lo:hi]
            copies.append(pltpu.make_async_copy(made.at[i, lo:hi], new.at[lo:hi], sems.at[i, j]))
            copies[-1].start()
    for copy in copies:
        copy.wait()


def shifted(block, axis, distance):
    count = lax.axis_size(axis)
    return lax.ppermute(block, axis, [(i - distance, i) for i in range(count) if 0 <= i - distance < count])


def local(increment, dual_state, forcing, gradient, courant_x, courant_y, error_var, obs_weight, diffusion, level_mix):
    _, L, X, Y = increment.shape
    assert Y == LANES and X % 8 == 0 and X > 2 * H and PITCH * (X + 2 * H) + 2 * H <= 2 * LANES
    LP = -(-L // 16) * 16
    flat = lambda t: t.reshape(L * X, Y)
    block = lambda t: t.reshape(L, X, Y)
    v, d = flat(increment), flat(dual_state)
    plane = lambda n: sds(n, LP, LANES)
    wide = lambda n: sds(n, LP, 2 * LANES)
    packed = lambda n: sds(n * L, LANES)
    natural = sds(L * X, Y)
    single = sds(LP, LANES)
    seam = sds(LP, 2 * LANES)
    matrix = sds(2 * LP, LP, dtype=BF16)
    scratch = lambda n: pltpu.VMEM((n, LP, LANES), F32)
    bind = lambda body, *sizes: functools.partial(body, *sizes)
    windows = lax.axis_size("tm")
    forward, backward = range(windows - 1), range(1, windows)

    dual_later = shifted(dual_state, "tm", -1)
    landing = [pltpu.VMEM((L, X + 8, LANES), F32)] * 3 + [pltpu.SemaphoreType.DMA((3, 4))]
    fields = (block(increment), block(courant_x), block(courant_y))
    opening = call(start_body, sds(8, LANES), (), flops=START_FLOPS)
    rows = call(
        bind(edges_body, X, L), (packed(3 * H - 2), packed(3 * H - 2), plane(H), plane(H)),
        fields + (block(dual_state), diffusion[None, :], opening),
        landing[:3] + [pltpu.VMEM((1, L), F32)] + landing[3:] + [pltpu.SemaphoreType.DMA],
        hbm=range(5), grant=EDGES_GRANT)
    halo = exchange(rows[0], rows[1], "gx", forward)
    uhalo = exchange(rows[2], rows[3], "gx", backward)
    tv, ta, tb, mats, matst, sb, ecore, mid = call(
        only(early, bind(core_body, X, L)),
        (plane(X),) * 3 + (matrix, matrix, single, packed(X - 2 * H), plane(8)),
        fields + (level_mix, diffusion[None, :]), [scratch(X), scratch(X)] + landing, hbm=range(3))
    ecore = shifted(ecore, "tm", 1)
    own, uown = call(bind(gather_body, X, L), (wide(6), wide(2)), (tv, ta, tb, d))
    uhalo, uyfirst, uysecond = call(
        only(late, bind(upack_body, X, L)), (packed(2 * H), seam, seam), (*uhalo, uown), [scratch(2 * H)])
    uhalo = shifted(uhalo, "tm", -1)
    ufrom = exchange(uyfirst, uysecond, "gy", backward)
    rd, ri, dk, ik, sums = call(
        base_body, (natural,) * 4 + (sds(2, 8, LANES),),
        (flat(forcing), flat(error_var), d, v, flat(gradient), flat(obs_weight)))

    top, bot, full, yfirst, ysecond = call(
        only(early, bind(pack_body, X)),
        (plane(3 * H - 2), plane(3 * H - 2), wide(6), seam, seam), (*halo, own, sb))
    sides = exchange(yfirst, ysecond, "gy", forward)
    erim = call(
        only(early, bind(rim_body, X, L)), packed(2 * H), (tv, ta, tb, top, bot, mid, sb, mats))
    erim = shifted(erim, "tm", 1)
    tfirst, tsecond, coef = call(
        bind(seam_body, X), (single, single, wide(4)), (full, *sides, *ufrom, sb, mats))
    seams = exchange(tfirst, tsecond, "tm")

    bcore, bmid, dual_own = call(
        only(early, bind(adjoint_core_body, X, L)),
        (plane(X - 2 * H), plane(4 * H), wide(2)),
        (block(dual_later), ta, tb, sb, matst), [scratch(H * X), scratch(H * X), landing[0], landing[3]],
        hbm=(0,))
    brim = call(
        only(early, bind(adjoint_rim_body, X, L)), plane(2 * H), (uhalo, bmid, ta, tb, top, bot, sb, matst))
    bseam = call(
        only(early, bind(adjoint_seam_body, X, L)), single, (uhalo, *seams, dual_own, coef, sb, matst))

    axes = ("tm", "gx", "gy")
    devices = lax.axis_size(axes)
    rdual, rincr, part = call(
        bind(residual_body, X, L), (natural, natural, sds(devices, LANES)),
        (ecore, erim, *seams, bcore, brim, bseam, rd, ri, sums), [pltpu.VMEM((2, 1, LANES), F32)])
    parts = lax.all_to_all(part, axes, 0, 0)
    count = 2 * increment.size * devices
    dnext, inext = call(
        bind(update_body, count), (natural, natural), (parts, dk, ik, rdual, rincr),
        [pltpu.VMEM((2, L * X, Y), F32), pltpu.SemaphoreType.DMA((2, 4))], outs_hbm=True)
    return dnext.reshape(increment.shape), inext.reshape(increment.shape)


def exchange(first, second, axis, windows=None):
    count = lax.axis_size(axis)
    out = []
    for turn, block in enumerate((first, second)):
        starts = range(turn, count - 1, 2)
        route = [pair for i in starts for pair in ((i, i + 1), (i + 1, i))]
        if not route:
            out.append(out[0])
            continue
        if windows is None:
            out.append(lax.ppermute(block, axis, route))
        else:
            wide = [(w * count + i, w * count + j) for w in windows for i, j in route]
            out.append(lax.ppermute(block, ("tm", axis), wide))
    return out


def solution(mesh):
    field = P("tm", None, "gx", "gy")
    return jax.shard_map(
        local, mesh=mesh, in_specs=(field,) * 8 + (P(), P()), out_specs=(field, field), check_vma=False)
```
